32 devices in a mesh: grp: 4 (over z), dev: 8 (over y, x, core).
Axes of the slice: x: 2, y: 2, z: 4, core: 2. Of those that a mesh axis runs over, the one named last changes fastest.
Arguments:
- blocks: bfloat16 [4096, 128, 128], P(('grp', 'dev')), may hold values from -0.29882812 to 0.29882812
- ids_one: int32 [2, 4096], P(None, ('grp', 'dev')), may hold values from 0 to 255, as said below
- ids_two: int32 [2, 2048], P(None, ('grp', 'dev')), may hold values from 0 to 127, as said below
- ids_three: int32 [2, 1024], P(None, ('grp', 'dev')), may hold values from 0 to 63
- match_one: int32 [256, 128], replicated, may hold values from 0 to 127, as said below
- match_two: int32 [128, 128], replicated, may hold values from 0 to 127, as said below
- match_three: int32 [64, 128], replicated, may hold values from 0 to 127, as said below
- target_one: int32 [4096], P(('grp', 'dev')), may hold values from 0 to 63
- target_two: int32 [2048], P(('grp', 'dev')), may hold values from 0 to 31
- target_three: int32 [1024], P(('grp', 'dev')), may hold values from 0 to 15
- vertex_weights: float32 [256, 128], P(('grp', 'dev')), may hold values from 0.1 to 120, as said below
Outputs:
- coarse_graph: float32 [512, 128, 128], P(('grp', 'dev'))
- rel_weight: float32 [32, 128], P(('grp', 'dev'))
The draws below stay inside these ranges and needn't reach their ends.
Inputs may be any that keep to these rules, and one draw needn't show every extreme that they name: `match_one`: rows 2b and 2b + 1 together name every number 0 to 127 exactly twice. `match_two`: rows 2b and 2b + 1 together name every number 0 to 127 exactly twice. `match_three`: rows 2b and 2b + 1 together name every number 0 to 127 exactly twice. `ids_one`: a fine block's row and column vertex blocks, halved by integer division, are the ids_two of the coarse slot it goes to. `ids_two`: a first-level block's row and column vertex blocks, halved by integer division, are the ids_three of the coarse slot it goes to. `vertex_weights`: positive.
All inputs are finite; a program needn't handle non-finite values.
Results may differ from the reference program's by a relative error of at most 0.0003.
Values may be sent and summed in bfloat16 or wider, within the bound.
A program may use at most 128 MiB of HBM per device.

```python
import math
import jax
import jax.numpy as jnp
from jax import lax

BLOCK = 128
SLOTS = 128
VWB = 8
NFINE = 4096
N_GRP = 4
N_DEV = 8
DEVICES = 32


def pairing(key, count):
    keys = jax.random.split(key, count // 2)
    perms = jax.vmap(lambda single: jax.random.permutation(single, 2 * BLOCK))(keys)
    return (perms // 2).reshape(count, BLOCK).astype(jnp.int32)


def route(count, per_dev, targets):
    slot = jnp.arange(count, dtype=jnp.int32)
    device = slot // per_dev
    local = slot % per_dev
    owner = device // N_DEV * N_DEV + local // (per_dev // N_DEV)
    return (owner * (per_dev // 2) + targets).astype(jnp.int32)


def layout(key):
    keys = jax.random.split(jax.random.fold_in(key, 7), 6)
    nfine = SLOTS * DEVICES
    vbzero = VWB * DEVICES
    ids_three = jax.random.randint(keys[0], (2, nfine // 4), 0, vbzero // 4, dtype=jnp.int32)
    target_two = jax.random.randint(keys[1], (nfine // 2,), 0, SLOTS // 4, dtype=jnp.int32)
    dest_two = route(nfine // 2, SLOTS // 2, target_two)
    ids_two = 2 * ids_three[:, dest_two] + jax.random.randint(keys[2], (2, nfine // 2), 0, 2, dtype=jnp.int32)
    target_one = jax.random.randint(keys[3], (nfine,), 0, SLOTS // 2, dtype=jnp.int32)
    dest_one = route(nfine, SLOTS, target_one)
    ids_one = 2 * ids_two[:, dest_one] + jax.random.randint(keys[4], (2, nfine), 0, 2, dtype=jnp.int32)
    target_three = jax.random.randint(keys[5], (nfine // 4,), 0, SLOTS // 8, dtype=jnp.int32)
    return (ids_one.astype(jnp.int32), ids_two.astype(jnp.int32), ids_three.astype(jnp.int32), target_one, target_two, target_three)


def draw_ids_one(key, part):
    return layout(key)[0]


def draw_ids_two(key, part):
    return layout(key)[1]


def draw_ids_three(key, part):
    return layout(key)[2]


def draw_target_one(key, part):
    return layout(key)[3]


def draw_target_two(key, part):
    return layout(key)[4]


def draw_target_three(key, part):
    return layout(key)[5]


def draw_match_one(key, part):
    return pairing(jax.random.fold_in(key, 11), VWB * DEVICES)


def draw_match_two(key, part):
    return pairing(jax.random.fold_in(key, 12), VWB * DEVICES // 2)


def draw_match_three(key, part):
    return pairing(jax.random.fold_in(key, 13), VWB * DEVICES // 4)


def draw_vertex_weights(key, part):
    first, second = jax.random.split(jax.random.fold_in(key, 21))
    count = VWB * DEVICES
    scale = jnp.exp(jax.random.uniform(first, (count, 1), jnp.float32, 0.0, math.log(16.0)))
    values = jax.random.uniform(second, (count, BLOCK), jnp.float32, 0.5, 1.5)
    return (scale * values).astype(jnp.float32)


def block_levels(own_key, extent, cuts, least, high):
    level = 1.0
    for position, shards_of in cuts:
        draws = jax.random.uniform(jax.random.fold_in(jax.random.fold_in(own_key, 6), position), (shards_of,), jnp.float32, least / len(cuts), high / len(cuts))
        level = level * jnp.repeat(jnp.exp(draws), extent[position] // shards_of).reshape((-1,) + (1,) * (len(extent) - 1 - position))
    return level


def scatter_about(own_key, dims, spread, reach, shards=(), kind=jnp.bfloat16):
    array = jax.random.normal(own_key, dims, jnp.float32) * spread
    if len(shards) > 0:
        array = block_levels(own_key, dims, shards, -0.22, 0.18) * array
    return jnp.clip(array, min=-reach, max=reach).astype(kind)


def setup_inputs(seed: int = 0) -> dict:
    key_list = jax.random.split(jax.random.key(seed), 12)
    return {
        "blocks": scatter_about(key_list[0], (NFINE, BLOCK, BLOCK), 0.05, 0.29882812, ((0, 32),)),
        "ids_one": draw_ids_one(jax.random.fold_in(key_list[11], 71), 0),
        "ids_two": draw_ids_two(jax.random.fold_in(key_list[11], 71), 0),
        "ids_three": draw_ids_three(jax.random.fold_in(key_list[11], 71), 0),
        "match_one": draw_match_one(jax.random.fold_in(key_list[11], 71), 0),
        "match_two": draw_match_two(jax.random.fold_in(key_list[11], 71), 0),
        "match_three": draw_match_three(jax.random.fold_in(key_list[11], 71), 0),
        "target_one": draw_target_one(jax.random.fold_in(key_list[11], 71), 0),
        "target_two": draw_target_two(jax.random.fold_in(key_list[11], 71), 0),
        "target_three": draw_target_three(jax.random.fold_in(key_list[11], 71), 0),
        "vertex_weights": draw_vertex_weights(jax.random.fold_in(key_list[11], 71), 0),
    }


def project_blocks(blocks, pair_ids, table):
    row_map = table[pair_ids[0]]
    col_map = table[pair_ids[1]]

    def single(matrix, rows, cols):
        halfway = jax.ops.segment_sum(matrix.astype(jnp.float32), rows, num_segments=BLOCK)
        return jax.ops.segment_sum(halfway.T, cols, num_segments=BLOCK).T

    return jax.vmap(single)(blocks, row_map, col_map)


def coarsen(blocks, pair_ids, table, targets, per_dev, fold_groups):
    count = blocks.shape[0]
    slot = jnp.arange(count, dtype=jnp.int32)
    device = slot // per_dev
    local = slot % per_dev
    group = device // N_DEV
    member = device % N_DEV
    if fold_groups:
        owner = (local // (per_dev // N_GRP)) * N_DEV + member
    else:
        owner = group * N_DEV + local // (per_dev // N_DEV)
    dest = (owner * (per_dev // 2) + targets).astype(jnp.int32)
    width = math.gcd(count, 512)
    turns = count // width
    inputs = (blocks.reshape(turns, width, BLOCK, BLOCK),
              pair_ids.reshape(2, turns, width).transpose(1, 0, 2),
              dest.reshape(turns, width))

    def accumulate(total, piece):
        part = project_blocks(piece[0], piece[1], table)
        return total.at[piece[2]].add(part), None

    start = jnp.zeros((count // 2, BLOCK, BLOCK), jnp.float32)
    coarse, _ = lax.scan(accumulate, start, inputs)
    return coarse


def pair_weights(weights, table):
    count = weights.shape[0]
    index = (jnp.arange(count, dtype=jnp.int32)[:, None] // 2) * BLOCK + table.astype(jnp.int32)
    summed = jax.ops.segment_sum(weights.reshape(-1), index.reshape(-1), num_segments=count // 2 * BLOCK)
    return summed.reshape(count // 2, BLOCK)


def reference(blocks, ids_one, ids_two, ids_three, match_one, match_two, match_three, target_one, target_two, target_three, vertex_weights):
    coarse_one = coarsen(blocks, ids_one, match_one, target_one, SLOTS, False)
    coarse_two = coarsen(coarse_one, ids_two, match_two, target_two, SLOTS // 2, False)
    coarse_graph = coarsen(coarse_two, ids_three, match_three, target_three, SLOTS // 4, True)
    weights_three = pair_weights(pair_weights(pair_weights(vertex_weights, match_one), match_two), match_three)
    total = jnp.sum(vertex_weights)
    rel_weight = weights_three * (weights_three.shape[0] * BLOCK) / total
    return coarse_graph, rel_weight
```

```python
import functools

import jax
import jax.numpy as jnp
from jax import lax
from jax.experimental import pallas as pl
from jax.experimental.pallas import tpu as pltpu
from jax.sharding import PartitionSpec as P

LEVELS = 32767.0
TINY = 1e-30
NT = (((1,), (1,)), ((), ()))


def hot(row, width):
    names = lax.broadcasted_iota(jnp.int32, (width, width), 0)
    return (names == row).astype(jnp.bfloat16)


def halves(x):
    high = x.astype(jnp.bfloat16)
    low = (x - high.astype(jnp.float32)).astype(jnp.bfloat16)
    return high, low


def columns(halfway, col):
    width = col.shape[1]
    right = hot(col, width)
    left = jnp.concatenate(halves(halfway), axis=1)
    both = jnp.concatenate([right, right], axis=1)
    return lax.dot_general(left, both, NT, preferred_element_type=jnp.float32)


def project_narrow(block, row, col):
    left = hot(row, row.shape[1])
    return columns(jnp.dot(left, block, preferred_element_type=jnp.float32), col)


def project_wide(block, row, col):
    left = hot(row, row.shape[1])
    both = jnp.concatenate([left, left], axis=1)
    stacked = jnp.concatenate(halves(block), axis=0)
    return columns(jnp.dot(both, stacked, preferred_element_type=jnp.float32), col)


def encode(part):
    peak = jnp.maximum(jnp.max(jnp.abs(part), axis=0, keepdims=True), TINY)
    code = jnp.round(part * (LEVELS / peak)).astype(jnp.int32)
    return code.astype(jnp.int16), peak * (1.0 / LEVELS)


def decode(code, scale):
    return code.astype(jnp.int32).astype(jnp.float32) * scale


def level_one(chunk, labels, ids, table, next_table, blocks, codes, scales, total):
    step = pl.program_id(0)

    @pl.when(step == 0)
    def _():
        total[...] = jnp.zeros_like(total)

    def several(start, count):
        parts = []
        for j in range(count):
            k = step * chunk + start + j
            row = table[pl.ds(labels[0, k], 1), :]
            col = table[pl.ds(labels[1, k], 1), :]
            parts.append(project_narrow(blocks[start + j], row, col))
        for j in range(count):
            k = step * chunk + start + j
            total[labels[2, k]] += parts[j]

    unroll = 4
    pl.loop(0, chunk // unroll)(lambda i: several(i * unroll, unroll))

    @pl.when(step == pl.num_programs(0) - 1)
    def _():
        send_parts(total, ids, next_table, codes, scales)


def send_parts(total, ids, table, codes, scales):
    unroll = 4

    def several(i):
        for j in range(unroll):
            k = i * unroll + j
            row = table[pl.ds(ids[0, k], 1), :]
            col = table[pl.ds(ids[1, k], 1), :]
            code, scale = encode(project_wide(total[k], row, col))
            codes[k] = code
            scales[k] = scale

    pl.loop(0, total.shape[0] // unroll)(several)


def level_two(targets, ids, table, codes_in, scales_in, codes, scales, total):
    total[...] = jnp.zeros_like(total)

    @pl.loop(0, codes_in.shape[0])
    def _(k):
        total[targets[k]] += decode(codes_in[k], scales_in[k])

    send_parts(total, ids, table, codes, scales)


def level_three(targets, codes_in, scales_in, total):
    total[...] = jnp.zeros_like(total)

    @pl.loop(0, codes_in.shape[0])
    def _(k):
        total[targets[k]] += decode(codes_in[k], scales_in[k])


SMEM = pl.BlockSpec(memory_space=pltpu.SMEM)
VMEM = pl.BlockSpec(memory_space=pltpu.VMEM)
PARAMS = pltpu.CompilerParams(vmem_limit_bytes=56 * 1024 * 1024)


def coded(count, width):
    return (
        jax.ShapeDtypeStruct((count, width, width), jnp.int16),
        jax.ShapeDtypeStruct((count, 1, width), jnp.float32),
    )


def pair_weights(weights, table_rows):
    count, width = weights.shape
    lanes = jnp.arange(width, dtype=jnp.int32)
    match = table_rows.reshape(count // 2, 2 * width)[:, :, None] == lanes
    spread = weights.reshape(count // 2, 2 * width)[:, :, None]
    return jnp.sum(jnp.where(match, spread, 0.0), axis=1)


def per_device(
    blocks,
    ids_one,
    ids_two,
    ids_three,
    match_one,
    match_two,
    match_three,
    target_one,
    target_two,
    target_three,
    vertex_weights,
):
    swap = functools.partial(lax.all_to_all, split_axis=0, concat_axis=0, tiled=True)
    count, width = blocks.shape[0], blocks.shape[1]
    labels = swap(jnp.stack([ids_one[0], ids_one[1], target_one], axis=1), "dev").T
    arrived_two = swap(target_two, "dev")
    arrived_three = swap(target_three, "grp")
    blocks = swap(blocks, "dev")
    chunk = 16
    codes, scales = pl.pallas_call(
        functools.partial(level_one, chunk),
        grid=(count // chunk,),
        in_specs=[
            SMEM,
            SMEM,
            VMEM,
            VMEM,
            pl.BlockSpec((chunk, width, width), lambda i: (i, 0, 0)),
        ],
        out_specs=(VMEM, VMEM),
        out_shape=coded(count // 2, width),
        scratch_shapes=[pltpu.VMEM((count // 2, width, width), jnp.float32)],
        compiler_params=PARAMS,
    )(labels, ids_two, match_one, match_two, blocks)
    codes, scales = swap(codes, "dev"), swap(scales, "dev")
    codes, scales = pl.pallas_call(
        level_two,
        in_specs=[SMEM, SMEM, VMEM, VMEM, VMEM],
        out_specs=(VMEM, VMEM),
        out_shape=coded(count // 4, width),
        scratch_shapes=[pltpu.VMEM((count // 4, width, width), jnp.float32)],
        compiler_params=PARAMS,
    )(arrived_two, ids_three, match_three, codes, scales)
    codes, scales = swap(codes, "grp"), swap(scales, "grp")
    coarse_graph = pl.pallas_call(
        level_three,
        in_specs=[SMEM, VMEM, VMEM],
        out_specs=VMEM,
        out_shape=jax.ShapeDtypeStruct((count // 8, width, width), jnp.float32),
        compiler_params=PARAMS,
    )(arrived_three, codes, scales)

    sums = lax.all_gather(jnp.sum(vertex_weights).reshape(1), ("grp", "dev"), tiled=True)
    total = jnp.sum(sums)
    owned = vertex_weights.shape[0]
    position = lax.axis_index(("grp", "dev"))
    weights = vertex_weights
    for table in (match_one, match_two, match_three):
        rows = lax.dynamic_slice_in_dim(table, position * owned, owned, 0)
        weights = pair_weights(weights, rows)
        owned //= 2
    vertices = weights.shape[0] * lax.axis_size(("grp", "dev")) * weights.shape[1]
    return coarse_graph, weights * vertices / total


def solution(mesh):
    both = ("grp", "dev")
    return jax.shard_map(
        per_device,
        mesh=mesh,
        in_specs=(
            P(both, None, None),
            P(None, both),
            P(None, both),
            P(None, both),
            P(),
            P(),
            P(),
            P(both),
            P(both),
            P(both),
            P(both, None),
        ),
        out_specs=(P(both, None, None), P(both, None)),
        check_vma=False,
    )
```

```python
import functools
import math

import jax
import jax.numpy as jnp
from jax import lax
from jax.experimental import pallas as pl
from jax.experimental.pallas import tpu as pltpu
from jax.sharding import PartitionSpec as P

LEVELS = 32767.0
TINY = 1e-30
NT = (((1,), (1,)), ((), ()))


def hot(row, width):
    names = lax.broadcasted_iota(jnp.int32, (width, width), 0)
    return (names == row).astype(jnp.bfloat16)


def halves(x):
    high = x.astype(jnp.bfloat16)
    low = (x - high.astype(jnp.float32)).astype(jnp.bfloat16)
    return high, low


def columns(halfway, col):
    width = col.shape[1]
    right = hot(col, width)
    left = jnp.concatenate(halves(halfway), axis=1)
    both = jnp.concatenate([right, right], axis=1)
    return lax.dot_general(left, both, NT, preferred_element_type=jnp.float32)


def project_narrow(block, row, col):
    left = hot(row, row.shape[1])
    return columns(jnp.dot(left, block, preferred_element_type=jnp.float32), col)


def project_wide(block, row, col):
    left = hot(row, row.shape[1])
    both = jnp.concatenate([left, left], axis=1)
    stacked = jnp.concatenate(halves(block), axis=0)
    return columns(jnp.dot(both, stacked, preferred_element_type=jnp.float32), col)


def encode(part):
    peak = jnp.maximum(jnp.max(jnp.abs(part), axis=0, keepdims=True), TINY)
    code = jnp.round(part * (LEVELS / peak)).astype(jnp.int32)
    return code.astype(jnp.int16), peak * (1.0 / LEVELS)


def decode(code, scale):
    return code.astype(jnp.int32).astype(jnp.float32) * scale


def chain(targets, order):
    lanes = targets.shape[1]
    square = (lanes, lanes)
    across = jnp.broadcast_to(targets, square)
    down = across.T
    order_across = jnp.broadcast_to(order, square)
    order_down = order_across.T
    earlier = (across == down) & (order_down < order_across)
    previous = jnp.max(jnp.where(earlier, order_down, -1), axis=0, keepdims=True)
    slots = lax.broadcasted_iota(jnp.int32, square, 1)
    last = jnp.max(jnp.where(down == slots, order_down, -1), axis=0, keepdims=True)
    return previous, last


def coarsen(
    n,
    groups,
    ids_two,
    ids_three,
    blocks,
    labels,
    labels_far,
    weight,
    match_one,
    match_two,
    match_three,
    coarse,
    weight_total,
    land,
    land_labels,
    land_far,
    land_weight,
    near_weight,
    land_weight_far,
    plan,
    plan_smem,
    sums_one,
    out_two,
    out_scale_two,
    land_two,
    land_scale_two,
    sums_two,
    out_three,
    out_scale_three,
    land_three,
    land_scale_three,
    sums_three,
    near_send,
    near_recv,
    far_send,
    far_recv,
    local,
):
    me = lax.axis_index("dev")
    group = lax.axis_index("grp")
    per_one, per_two, per_three = land.shape[1], land_two.shape[1], land_three.shape[1]
    count_one, count_two, count_three = n * per_one, n * per_two, groups * per_three

    def peer(step):
        return lax.rem(me + step, n)

    def source(step):
        return lax.rem(me - step + n, n)

    def far_peer(step):
        return lax.rem(group + step, groups)

    def far_source(step):
        return lax.rem(group - step + groups, groups)

    def near(kind, src, dst, there, here):
        return pltpu.make_async_remote_copy(
            src_ref=src,
            dst_ref=dst,
            send_sem=near_send.at[kind, there],
            recv_sem=near_recv.at[kind, here],
            device_id={"dev": there},
            device_id_type=pl.DeviceIdType.MESH,
        )

    def far(kind, src, dst, there, here):
        return pltpu.make_async_remote_copy(
            src_ref=src,
            dst_ref=dst,
            send_sem=far_send.at[kind, there],
            recv_sem=far_recv.at[kind, here],
            device_id={"grp": there},
            device_id_type=pl.DeviceIdType.MESH,
        )

    def send_labels(v, here):
        return near(0, labels.at[v], land_labels.at[here], v, here)

    def send_weight(v, here):
        return near(1, weight, land_weight.at[here], v, here)

    def send_blocks(v, here):
        return near(2, blocks.at[v], land.at[here], v, here)

    def send_codes(v, here):
        return near(3, out_two.at[v], land_two.at[here], v, here)

    def send_scales(v, here):
        return near(4, out_scale_two.at[v], land_scale_two.at[here], v, here)

    def send_labels_far(v, here):
        return far(0, labels_far.at[v], land_far.at[here], v, here)

    def send_weight_far(v, here):
        return far(1, near_weight, land_weight_far.at[here], v, here)

    def send_codes_far(v, here):
        return far(2, out_three.at[v], land_three.at[here], v, here)

    def send_scales_far(v, here):
        return far(3, out_scale_three.at[v], land_scale_three.at[here], v, here)

    near_kinds = (send_labels, send_weight, send_blocks, send_codes, send_scales)
    far_kinds = (send_labels_far, send_weight_far, send_codes_far, send_scales_far)

    own_blocks = pltpu.make_async_copy(blocks.at[me], land.at[me], local.at[0])
    own_blocks.start()
    own_labels = pltpu.make_async_copy(labels.at[me], land_labels.at[me], local.at[1])
    own_labels.start()
    own_far = pltpu.make_async_copy(labels_far.at[group], land_far.at[group], local.at[2])
    own_far.start()

    barrier = pltpu.get_barrier_semaphore()

    @pl.loop(1, n)
    def _(step):
        pl.semaphore_signal(
            barrier, inc=1, device_id={"dev": peer(step)}, device_id_type=pl.DeviceIdType.MESH
        )

    @pl.loop(1, groups)
    def _(step):
        pl.semaphore_signal(
            barrier, inc=1, device_id={"grp": far_peer(step)}, device_id_type=pl.DeviceIdType.MESH
        )

    pl.semaphore_wait(barrier, n + groups - 2)

    @pl.loop(1, n)
    def _(step):
        send_labels(peer(step), me).start()
        send_weight(peer(step), me).start()

    @pl.loop(1, groups)
    def _(step):
        send_labels_far(far_peer(step), group).start()

    @pl.loop(1, n)
    def _(step):
        send_blocks(peer(step), me).start()

    block_shape = sums_one.shape[1:]
    sums_one[count_one] = jnp.zeros(block_shape, jnp.float32)
    sums_two[count_two] = jnp.zeros(block_shape, jnp.float32)
    sums_three[count_three] = jnp.zeros(block_shape, jnp.float32)

    own_labels.wait()
    own_far.wait()

    @pl.loop(1, n)
    def _(step):
        send_labels(source(step), source(step)).wait_recv()
        send_weight(source(step), source(step)).wait_recv()

    @pl.loop(1, groups)
    def _(step):
        send_labels_far(far_source(step), far_source(step)).wait_recv()

    rows, lanes = plan.shape
    lane = lax.broadcasted_iota(jnp.int32, (rows, lanes), 1)

    def gathered(arrived, sources, per):
        def add(u, held):
            return held + jnp.where(lane // per == u, arrived[u], 0)

        return lax.fori_loop(0, sources, add, jnp.zeros((rows, lanes), jnp.int32))

    lane = lax.broadcasted_iota(jnp.int32, (rows, lanes), 1)
    one_row = lax.broadcasted_iota(jnp.int32, (1, lanes), 1)

    def order(position, sources, per):
        return lax.rem(position - one_row // per + sources, sources) * per + lax.rem(one_row, per)

    known = gathered(land_labels, n, per_one)
    known_two = gathered(land_labels, n, per_two)
    known_far = gathered(land_far, groups, per_three)
    inside_two = one_row < count_two
    inside_three = one_row < count_three
    previous_one, last_one = chain(known[2:3], order(me, n, per_one))
    previous_two, last_two = chain(
        jnp.where(inside_two, known_two[3:4], -1), jnp.where(inside_two, order(me, n, per_two), -1)
    )
    previous_three, last_three = chain(
        jnp.where(inside_three, known_far[0:1], -1),
        jnp.where(inside_three, order(group, groups, per_three), -1),
    )

    def settled(found, zero):
        return jnp.where(found < 0, zero, found)

    plan[0:1] = known[0:1]
    plan[1:2] = known[1:2]
    plan[2:3] = settled(previous_one, count_one)
    plan[3:4] = settled(last_one, count_one)
    plan[4:5] = settled(previous_two, count_two)
    plan[5:6] = settled(last_two, count_two)
    plan[6:7] = settled(previous_three, count_three)
    plan[7:8] = settled(last_three, count_three)
    to_smem = pltpu.make_async_copy(plan, plan_smem, local.at[3])
    to_smem.start()

    held = weight[...]
    for step in range(1, n):
        held = held + land_weight[source(step)]
    near_weight[...] = held
    to_smem.wait()

    def level_one(step):
        u = source(step)
        unroll = math.gcd(per_one, 4)

        @pl.loop(0, per_one // unroll)
        def _(i):
            parts = []
            for j in range(unroll):
                k = i * unroll + j
                row = match_one[pl.ds(plan_smem[0, u * per_one + k], 1), :]
                col = match_one[pl.ds(plan_smem[1, u * per_one + k], 1), :]
                parts.append(project_narrow(land[u, k], row, col))
            for j in range(unroll):
                k = i * unroll + j
                before = sums_one[plan_smem[2, u * per_one + k]]
                sums_one[step * per_one + k] = parts[j] + before

    own_blocks.wait()
    level_one(0)

    @pl.loop(1, n)
    def _(step):
        send_blocks(source(step), source(step)).wait_recv()
        level_one(step)

    def parts_out(v, per, plan_row, ids, table, sums, codes, scales):
        unroll = math.gcd(per, 4)

        @pl.loop(0, per // unroll)
        def _(i):
            parts = []
            for j in range(unroll):
                slot = v * per + i * unroll + j
                row = table[pl.ds(ids[0, slot], 1), :]
                col = table[pl.ds(ids[1, slot], 1), :]
                parts.append(project_wide(sums[plan_smem[plan_row, slot]], row, col))
            for j in range(unroll):
                code, scale = encode(parts[j])
                codes[v, i * unroll + j] = code
                scales[v, i * unroll + j] = scale

    def parts_in(step, u, per, plan_row, codes, scales, sums):
        @pl.loop(0, per)
        def _(k):
            before = sums[plan_smem[plan_row, u * per + k]]
            sums[step * per + k] = decode(codes[u, k], scales[u, k]) + before

    @pl.loop(1, n)
    def _(step):
        v = peer(step)
        parts_out(v, per_two, 3, ids_two, match_two, sums_one, out_two, out_scale_two)
        send_codes(v, me).start()
        send_scales(v, me).start()

    parts_out(me, per_two, 3, ids_two, match_two, sums_one, out_two, out_scale_two)
    parts_in(0, me, per_two, 4, out_two, out_scale_two, sums_two)

    @pl.loop(1, groups)
    def _(step):
        send_weight_far(far_peer(step), group).start()

    @pl.loop(1, n)
    def _(step):
        u = source(step)
        send_codes(u, u).wait_recv()
        send_scales(u, u).wait_recv()
        parts_in(step, u, per_two, 4, land_two, land_scale_two, sums_two)

    @pl.loop(1, groups)
    def _(step):
        v = far_peer(step)
        parts_out(v, per_three, 5, ids_three, match_three, sums_two, out_three, out_scale_three)
        send_codes_far(v, group).start()
        send_scales_far(v, group).start()

    parts_out(group, per_three, 5, ids_three, match_three, sums_two, out_three, out_scale_three)
    parts_in(0, group, per_three, 6, out_three, out_scale_three, sums_three)

    held = near_weight[...]
    for step in range(1, groups):
        send_weight_far(far_source(step), far_source(step)).wait_recv()
        held = held + land_weight_far[far_source(step)]
    weight_total[...] = held

    @pl.loop(1, groups)
    def _(step):
        u = far_source(step)
        send_codes_far(u, u).wait_recv()
        send_scales_far(u, u).wait_recv()
        parts_in(step, u, per_three, 6, land_three, land_scale_three, sums_three)

    @pl.loop(0, coarse.shape[0])
    def _(slot):
        coarse[slot] = sums_three[plan_smem[7, slot]]

    @pl.loop(1, n)
    def _(step):
        for kind in near_kinds:
            kind(peer(step), me).wait_send()

    @pl.loop(1, groups)
    def _(step):
        for kind in far_kinds:
            kind(far_peer(step), group).wait_send()


SMEM = pl.BlockSpec(memory_space=pltpu.SMEM)
VMEM = pl.BlockSpec(memory_space=pltpu.VMEM)
HBM = pl.BlockSpec(memory_space=pl.ANY)
LANES, ROWS = 128, 8


def spread(values, parts, times):
    per = values.shape[0] // parts
    wide = jnp.tile(values.reshape(parts, per), (1, times))
    return jnp.pad(wide, ((0, 0), (0, LANES - times * per)))


def pair_weights(weights, table_rows):
    count, width = weights.shape
    lanes = jnp.arange(width, dtype=jnp.int32)
    match = table_rows.reshape(count // 2, 2 * width)[:, :, None] == lanes
    spread_out = weights.reshape(count // 2, 2 * width)[:, :, None]
    return jnp.sum(jnp.where(match, spread_out, 0.0), axis=1)


def per_device(
    blocks,
    ids_one,
    ids_two,
    ids_three,
    match_one,
    match_two,
    match_three,
    target_one,
    target_two,
    target_three,
    vertex_weights,
):
    n, groups = lax.axis_size("dev"), lax.axis_size("grp")
    count, width = blocks.shape[0], blocks.shape[1]
    rows = [spread(r, n, n) for r in (ids_one[0], ids_one[1], target_one, target_two)]
    labels = jnp.stack(rows + rows, axis=1)
    labels_far = jnp.stack([spread(target_three, groups, groups)] * ROWS, axis=1)
    weight = jnp.broadcast_to(jnp.sum(vertex_weights), (ROWS, LANES))
    per_one, per_two, per_three = count // n, count // 2 // n, count // 4 // groups
    block = (width, width)
    near_kinds, far_kinds = 5, 4
    coarse_graph, total = pl.pallas_call(
        functools.partial(coarsen, n, groups),
        in_specs=[SMEM, SMEM, HBM, VMEM, VMEM, VMEM, VMEM, VMEM, VMEM],
        out_specs=(VMEM, VMEM),
        out_shape=(
            jax.ShapeDtypeStruct((count // 8,) + block, jnp.float32),
            jax.ShapeDtypeStruct((ROWS, LANES), jnp.float32),
        ),
        scratch_shapes=[
            pltpu.VMEM((n, per_one) + block, jnp.bfloat16),
            pltpu.VMEM((n, ROWS, LANES), jnp.int32),
            pltpu.VMEM((groups, ROWS, LANES), jnp.int32),
            pltpu.VMEM((n, ROWS, LANES), jnp.float32),
            pltpu.VMEM((ROWS, LANES), jnp.float32),
            pltpu.VMEM((groups, ROWS, LANES), jnp.float32),
            pltpu.VMEM((ROWS, LANES), jnp.int32),
            pltpu.SMEM((ROWS, LANES), jnp.int32),
            pltpu.VMEM((count + 1,) + block, jnp.float32),
            pltpu.VMEM((n, per_two) + block, jnp.int16),
            pltpu.VMEM((n, per_two, 1, width), jnp.float32),
            pltpu.VMEM((n, per_two) + block, jnp.int16),
            pltpu.VMEM((n, per_two, 1, width), jnp.float32),
            pltpu.VMEM((count // 2 + 1,) + block, jnp.float32),
            pltpu.VMEM((groups, per_three) + block, jnp.int16),
            pltpu.VMEM((groups, per_three, 1, width), jnp.float32),
            pltpu.VMEM((groups, per_three) + block, jnp.int16),
            pltpu.VMEM((groups, per_three, 1, width), jnp.float32),
            pltpu.VMEM((count // 4 + 1,) + block, jnp.float32),
            pltpu.SemaphoreType.DMA((near_kinds, n)),
            pltpu.SemaphoreType.DMA((near_kinds, n)),
            pltpu.SemaphoreType.DMA((far_kinds, groups)),
            pltpu.SemaphoreType.DMA((far_kinds, groups)),
            pltpu.SemaphoreType.DMA((4,)),
        ],
        compiler_params=pltpu.CompilerParams(
            collective_id=0, has_side_effects=True, vmem_limit_bytes=60 * 1024 * 1024
        ),
    )(
        ids_two,
        ids_three,
        blocks.reshape((n, per_one) + block),
        labels,
        labels_far,
        weight,
        match_one,
        match_two,
        match_three,
    )
    owned = vertex_weights.shape[0]
    position = lax.axis_index("grp") * n + lax.axis_index("dev")
    weights = vertex_weights
    for table in (match_one, match_two, match_three):
        mine = lax.dynamic_slice_in_dim(table, position * owned, owned, 0)
        weights = pair_weights(weights, mine)
        owned //= 2
    vertices = weights.shape[0] * n * groups * weights.shape[1]
    return coarse_graph, weights * vertices / total[:1, :1]


def solution(mesh):
    both = ("grp", "dev")
    return jax.shard_map(
        per_device,
        mesh=mesh,
        in_specs=(
            P(both, None, None),
            P(None, both),
            P(None, both),
            P(None, both),
            P(),
            P(),
            P(),
            P(both),
            P(both),
            P(both),
            P(both, None),
        ),
        out_specs=(P(both, None, None), P(both, None)),
        check_vma=False,
    )
```

```python
import functools
import math

import jax
import jax.numpy as jnp
from jax import lax
from jax.experimental import pallas as pl
from jax.experimental.pallas import tpu as pltpu
from jax.sharding import PartitionSpec as P

LEVELS = 32767.0
TINY = 1e-30
NT = (((1,), (1,)), ((), ()))


def hot(row, width):
    names = lax.broadcasted_iota(jnp.int32, (width, width), 0)
    return (names == row).astype(jnp.bfloat16)


def halves(x):
    high = x.astype(jnp.bfloat16)
    low = (x - high.astype(jnp.float32)).astype(jnp.bfloat16)
    return high, low


def columns(halfway, col):
    width = col.shape[1]
    right = hot(col, width)
    left = jnp.concatenate(halves(halfway), axis=1)
    both = jnp.concatenate([right, right], axis=1)
    return lax.dot_general(left, both, NT, preferred_element_type=jnp.float32)


def project_narrow(block, row, col):
    left = hot(row, row.shape[1])
    return columns(jnp.dot(left, block, preferred_element_type=jnp.float32), col)


def project_wide(block, row, col):
    left = hot(row, row.shape[1])
    both = jnp.concatenate([left, left], axis=1)
    stacked = jnp.concatenate(halves(block), axis=0)
    return columns(jnp.dot(both, stacked, preferred_element_type=jnp.float32), col)


def encode(part):
    peak = jnp.maximum(jnp.max(jnp.abs(part), axis=0, keepdims=True), TINY)
    code = jnp.round(part * (LEVELS / peak)).astype(jnp.int32)
    return code.astype(jnp.int16), peak * (1.0 / LEVELS)


def decode(code, scale):
    return code.astype(jnp.int32).astype(jnp.float32) * scale


def fold(weights, row):
    width = row.shape[1]
    right = hot(row, width)
    rest = jnp.broadcast_to(weights, (8, width))
    total = jnp.zeros((8, width), jnp.float32)
    for _ in range(3):
        part = rest.astype(jnp.bfloat16)
        rest = rest - part.astype(jnp.float32)
        total = total + lax.dot_general(part, right, NT, preferred_element_type=jnp.float32)
    return total[:1]


def chain(arrived, label, sources, per, mine, lanes):
    square = (lanes, lanes)
    count = sources * per
    down_at = lax.broadcasted_iota(jnp.int32, square, 0)
    across_at = lax.broadcasted_iota(jnp.int32, square, 1)
    sender, local_slot = down_at // per, down_at % per

    def add(u, held):
        row = jnp.broadcast_to(arrived[u, label : label + 1, :], square)
        return jnp.where(sender == u, row, held)

    held = lax.fori_loop(0, sources, add, jnp.zeros(square, jnp.int32))
    picked = jnp.where(across_at == mine * per + local_slot, held, 0)
    down = jnp.broadcast_to(jnp.sum(picked, axis=1, keepdims=True), square)
    down = jnp.where(down_at < count, down, -1)
    order_down = (mine - sender + sources) % sources * per + local_slot
    order_across = (mine - across_at // per + sources) % sources * per + across_at % per
    earlier = (down.T == down) & (order_down < order_across) & (down_at < count)
    previous = jnp.max(jnp.where(earlier, order_down, -1), axis=0, keepdims=True)
    last = jnp.max(jnp.where(down == across_at, order_down, -1), axis=0, keepdims=True)
    return jnp.where(previous < 0, count, previous), jnp.where(last < 0, count, last)


def coarsen(
    n,
    groups,
    ids_two,
    ids_three,
    blocks,
    labels,
    weight,
    match_one,
    match_two,
    match_three,
    coarse,
    relative,
    land,
    land_labels,
    land_far,
    land_weight,
    near_weight,
    land_weight_far,
    plan,
    plan_smem,
    labels_smem,
    coarse_weight,
    sums_one,
    out_two,
    out_scale_two,
    land_two,
    land_scale_two,
    sums_two,
    out_three,
    out_scale_three,
    land_three,
    land_scale_three,
    sums_three,
    near_send,
    near_recv,
    far_send,
    far_recv,
    local,
):
    me = lax.axis_index("dev")
    group = lax.axis_index("grp")
    per_one, per_two, per_three = land.shape[1], land_two.shape[1], land_three.shape[1]
    count_one, count_two, count_three = n * per_one, n * per_two, groups * per_three

    def peer(step):
        return lax.rem(me + step, n)

    def source(step):
        return lax.rem(me - step + n, n)

    def far_peer(step):
        return lax.rem(group + step, groups)

    def far_source(step):
        return lax.rem(group - step + groups, groups)

    def near(kind, src, dst, there, here):
        return pltpu.make_async_remote_copy(
            src_ref=src,
            dst_ref=dst,
            send_sem=near_send.at[kind, there],
            recv_sem=near_recv.at[kind, here],
            device_id={"dev": there},
            device_id_type=pl.DeviceIdType.MESH,
        )

    def far(kind, src, dst, there, here):
        return pltpu.make_async_remote_copy(
            src_ref=src,
            dst_ref=dst,
            send_sem=far_send.at[kind, there],
            recv_sem=far_recv.at[kind, here],
            device_id={"grp": there},
            device_id_type=pl.DeviceIdType.MESH,
        )

    def send_labels(v, here):
        return near(0, labels, land_labels.at[here], v, here)

    def send_weight(v, here):
        return near(1, weight, land_weight.at[here], v, here)

    def send_blocks(v, here):
        return near(2, blocks.at[v], land.at[here], v, here)

    def send_codes(v, here):
        return near(3, out_two.at[v], land_two.at[here], v, here)

    def send_scales(v, here):
        return near(4, out_scale_two.at[v], land_scale_two.at[here], v, here)

    def send_labels_far(v, here):
        return far(0, labels, land_far.at[here], v, here)

    def send_weight_far(v, here):
        return far(1, near_weight, land_weight_far.at[here], v, here)

    def send_codes_far(v, here):
        return far(2, out_three.at[v], land_three.at[here], v, here)

    def send_scales_far(v, here):
        return far(3, out_scale_three.at[v], land_scale_three.at[here], v, here)

    near_kinds = (send_labels, send_weight, send_blocks, send_codes, send_scales)
    far_kinds = (send_labels_far, send_weight_far, send_codes_far, send_scales_far)

    own_blocks = pltpu.make_async_copy(blocks.at[me], land.at[me], local.at[0])
    own_blocks.start()
    own_labels = pltpu.make_async_copy(labels, land_labels.at[me], local.at[1])
    own_labels.start()
    own_far = pltpu.make_async_copy(labels, land_far.at[group], local.at[2])
    own_far.start()

    barrier = pltpu.get_barrier_semaphore()

    @pl.loop(1, n)
    def _(step):
        pl.semaphore_signal(
            barrier, inc=1, device_id={"dev": peer(step)}, device_id_type=pl.DeviceIdType.MESH
        )

    @pl.loop(1, groups)
    def _(step):
        pl.semaphore_signal(
            barrier, inc=1, device_id={"grp": far_peer(step)}, device_id_type=pl.DeviceIdType.MESH
        )

    pl.semaphore_wait(barrier, n + groups - 2)

    @pl.loop(1, n)
    def _(step):
        send_labels(peer(step), me).start()
        send_weight(peer(step), me).start()

    @pl.loop(1, groups)
    def _(step):
        send_labels_far(far_peer(step), group).start()

    @pl.loop(1, n)
    def _(step):
        send_blocks(peer(step), me).start()

    block_shape = sums_one.shape[1:]
    sums_one[count_one] = jnp.zeros(block_shape, jnp.float32)
    sums_two[count_two] = jnp.zeros(block_shape, jnp.float32)
    sums_three[count_three] = jnp.zeros(block_shape, jnp.float32)

    own_labels.wait()
    own_far.wait()

    @pl.loop(1, n)
    def _(step):
        send_labels(source(step), source(step)).wait_recv()
        send_weight(source(step), source(step)).wait_recv()

    @pl.loop(1, groups)
    def _(step):
        send_labels_far(far_source(step), far_source(step)).wait_recv()

    labels_down = pltpu.make_async_copy(land_labels, labels_smem, local.at[4])
    labels_down.start()
    lanes = plan.shape[1]
    levels = (
        (land_labels, 2, n, per_one, me),
        (land_labels, 3, n, per_two, me),
        (land_far, 4, groups, per_three, group),
    )
    for level, (arrived, label, sources, per, mine) in enumerate(levels):
        previous, last = chain(arrived, label, sources, per, mine, lanes)
        plan[2 * level + 2 : 2 * level + 3] = previous
        plan[2 * level + 3 : 2 * level + 4] = last
    to_smem = pltpu.make_async_copy(plan, plan_smem, local.at[3])
    to_smem.start()

    held = weight[...]
    for step in range(1, n):
        held = held + land_weight[peer(step)]
    near_weight[...] = held
    position = group * n + me
    owned = [weight[e : e + 1, :] for e in range(weight.shape[0])]
    for table in (match_one, match_two, match_three):
        base = position * len(owned)
        folded = [fold(w, table[pl.ds(base + e, 1), :]) for e, w in enumerate(owned)]
        owned = [folded[e] + folded[e + 1] for e in range(0, len(folded), 2)]
    for e, w in enumerate(owned):
        coarse_weight[e : e + 1, :] = w
    labels_down.wait()
    to_smem.wait()

    def level_one(step):
        u = source(step)
        unroll = math.gcd(per_one, 4)

        @pl.loop(0, per_one // unroll)
        def _(i):
            parts = []
            for j in range(unroll):
                k = i * unroll + j
                row = match_one[pl.ds(labels_smem[u, 0, me * per_one + k], 1), :]
                col = match_one[pl.ds(labels_smem[u, 1, me * per_one + k], 1), :]
                parts.append(project_narrow(land[u, k], row, col))
            for j in range(unroll):
                k = i * unroll + j
                before = sums_one[plan_smem[2, u * per_one + k]]
                sums_one[step * per_one + k] = parts[j] + before

    own_blocks.wait()
    level_one(0)

    @pl.loop(1, n)
    def _(step):
        send_blocks(source(step), source(step)).wait_recv()
        level_one(step)

    def parts_out(v, per, plan_row, ids, table, sums, codes, scales):
        unroll = math.gcd(per, 4)

        @pl.loop(0, per // unroll)
        def _(i):
            parts = []
            for j in range(unroll):
                slot = v * per + i * unroll + j
                row = table[pl.ds(ids[0, slot], 1), :]
                col = table[pl.ds(ids[1, slot], 1), :]
                parts.append(project_wide(sums[plan_smem[plan_row, slot]], row, col))
            for j in range(unroll):
                code, scale = encode(parts[j])
                codes[v, i * unroll + j] = code
                scales[v, i * unroll + j] = scale

    def parts_in(step, u, per, plan_row, codes, scales, sums):
        @pl.loop(0, per)
        def _(k):
            before = sums[plan_smem[plan_row, u * per + k]]
            sums[step * per + k] = decode(codes[u, k], scales[u, k]) + before

    @pl.loop(1, n)
    def _(step):
        v = peer(step)
        parts_out(v, per_two, 3, ids_two, match_two, sums_one, out_two, out_scale_two)
        send_codes(v, me).start()
        send_scales(v, me).start()

    parts_out(me, per_two, 3, ids_two, match_two, sums_one, out_two, out_scale_two)
    parts_in(0, me, per_two, 4, out_two, out_scale_two, sums_two)

    @pl.loop(1, groups)
    def _(step):
        send_weight_far(far_peer(step), group).start()

    @pl.loop(1, n)
    def _(step):
        u = source(step)
        send_codes(u, u).wait_recv()
        send_scales(u, u).wait_recv()
        parts_in(step, u, per_two, 4, land_two, land_scale_two, sums_two)

    @pl.loop(1, groups)
    def _(step):
        v = far_peer(step)
        parts_out(v, per_three, 5, ids_three, match_three, sums_two, out_three, out_scale_three)
        send_codes_far(v, group).start()
        send_scales_far(v, group).start()

    parts_out(group, per_three, 5, ids_three, match_three, sums_two, out_three, out_scale_three)
    parts_in(0, group, per_three, 6, out_three, out_scale_three, sums_three)

    held = near_weight[...]
    for step in range(1, groups):
        send_weight_far(far_source(step), far_source(step)).wait_recv()
        held = held + land_weight_far[far_source(step)]
    total = jnp.sum(jnp.sum(held, axis=0, keepdims=True), axis=1, keepdims=True)
    vertices = relative.shape[0] * n * groups * relative.shape[1]
    relative[...] = coarse_weight[...] * vertices / total

    @pl.loop(1, groups)
    def _(step):
        u = far_source(step)
        send_codes_far(u, u).wait_recv()
        send_scales_far(u, u).wait_recv()
        parts_in(step, u, per_three, 6, land_three, land_scale_three, sums_three)

    @pl.loop(0, coarse.shape[0])
    def _(slot):
        coarse[slot] = sums_three[plan_smem[7, slot]]

    @pl.loop(1, n)
    def _(step):
        for kind in near_kinds:
            kind(peer(step), me).wait_send()

    @pl.loop(1, groups)
    def _(step):
        for kind in far_kinds:
            kind(far_peer(step), group).wait_send()


SMEM = pl.BlockSpec(memory_space=pltpu.SMEM)
VMEM = pl.BlockSpec(memory_space=pltpu.VMEM)
HBM = pl.BlockSpec(memory_space=pl.ANY)
ROWS = 8


def per_device(
    blocks,
    ids_one,
    ids_two,
    ids_three,
    match_one,
    match_two,
    match_three,
    target_one,
    target_two,
    target_three,
    vertex_weights,
):
    n, groups = lax.axis_size("dev"), lax.axis_size("grp")
    count, width = blocks.shape[0], blocks.shape[1]
    lanes = -(-count // width) * width
    rows = (ids_one, target_one[None], target_two[None], target_three[None])
    held = [jnp.pad(r, ((0, 0), (0, lanes - r.shape[1]))) for r in rows]
    labels = jnp.pad(jnp.concatenate(held), ((0, ROWS - 5), (0, 0)))
    owned = vertex_weights.shape[0]
    per_one, per_two, per_three = count // n, count // 2 // n, count // 4 // groups
    block = (width, width)
    near_kinds, far_kinds = 5, 4
    return pl.pallas_call(
        functools.partial(coarsen, n, groups),
        in_specs=[SMEM, SMEM, HBM, VMEM, VMEM, VMEM, VMEM, VMEM],
        out_specs=(VMEM, VMEM),
        out_shape=(
            jax.ShapeDtypeStruct((count // 8,) + block, jnp.float32),
            jax.ShapeDtypeStruct((owned // 8, width), jnp.float32),
        ),
        scratch_shapes=[
            pltpu.VMEM((n, per_one) + block, jnp.bfloat16),
            pltpu.VMEM((n, ROWS, lanes), jnp.int32),
            pltpu.VMEM((groups, ROWS, lanes), jnp.int32),
            pltpu.VMEM((n, owned, width), jnp.float32),
            pltpu.VMEM((owned, width), jnp.float32),
            pltpu.VMEM((groups, owned, width), jnp.float32),
            pltpu.VMEM((ROWS, lanes), jnp.int32),
            pltpu.SMEM((ROWS, lanes), jnp.int32),
            pltpu.SMEM((n, ROWS, lanes), jnp.int32),
            pltpu.VMEM((owned // 8, width), jnp.float32),
            pltpu.VMEM((count + 1,) + block, jnp.float32),
            pltpu.VMEM((n, per_two) + block, jnp.int16),
            pltpu.VMEM((n, per_two, 1, width), jnp.float32),
            pltpu.VMEM((n, per_two) + block, jnp.int16),
            pltpu.VMEM((n, per_two, 1, width), jnp.float32),
            pltpu.VMEM((count // 2 + 1,) + block, jnp.float32),
            pltpu.VMEM((groups, per_three) + block, jnp.int16),
            pltpu.VMEM((groups, per_three, 1, width), jnp.float32),
            pltpu.VMEM((groups, per_three) + block, jnp.int16),
            pltpu.VMEM((groups, per_three, 1, width), jnp.float32),
            pltpu.VMEM((count // 4 + 1,) + block, jnp.float32),
            pltpu.SemaphoreType.DMA((near_kinds, n)),
            pltpu.SemaphoreType.DMA((near_kinds, n)),
            pltpu.SemaphoreType.DMA((far_kinds, groups)),
            pltpu.SemaphoreType.DMA((far_kinds, groups)),
            pltpu.SemaphoreType.DMA((5,)),
        ],
        compiler_params=pltpu.CompilerParams(
            collective_id=0, has_side_effects=True, vmem_limit_bytes=60 * 1024 * 1024
        ),
    )(
        ids_two,
        ids_three,
        blocks.reshape((n, per_one) + block),
        labels,
        vertex_weights,
        match_one,
        match_two,
        match_three,
    )


def solution(mesh):
    both = ("grp", "dev")
    return jax.shard_map(
        per_device,
        mesh=mesh,
        in_specs=(
            P(both, None, None),
            P(None, both),
            P(None, both),
            P(None, both),
            P(),
            P(),
            P(),
            P(both),
            P(both),
            P(both),
            P(both, None),
        ),
        out_specs=(P(both, None, None), P(both, None)),
        check_vma=False,
    )
```
